32 devices in a mesh: ep: 8 (over z, x), tp: 4 (over y, core).
Axes of the slice: x: 2, y: 2, z: 4, core: 2. Of those that a mesh axis runs over, the one named last changes fastest.
Arguments:
- tokens: bfloat16 [2048, 2880], P('ep', 'tp'), may hold values from -6 to 6
- expert_ids: int32 [2048, 4], P('ep'), may hold values from 0 to 15, all different within a row; in each aligned block of 256 rows (0 to 255, 256 to 511, ...) at most 128 rows name the same one
- combine_weights: float32 [2048, 4], P('ep'), may hold values from 0.05 to 0.6
- gate_weight: bfloat16 [16, 2880, 2880], P('ep', None, 'tp'), may hold values from -0.109375 to 0.109375
- up_weight: bfloat16 [16, 2880, 2880], P('ep', None, 'tp'), may hold values from -0.109375 to 0.109375
- down_weight: bfloat16 [16, 2880, 2880], P('ep', 'tp'), may hold values from -0.109375 to 0.109375
Outputs:
- mixed: bfloat16 [2048, 2880], P('ep', 'tp')
The draws below stay inside these ranges and needn't reach their ends.
Inputs may be any that keep to these rules, and one draw needn't show every extreme that they name: `expert_ids`: each row names 4 different experts; within the 256 rows of one index of ep no expert is named more than 128 times, a bound that some block reaches.
All inputs are finite; a program needn't handle non-finite values.
Results may differ from the reference program's by a relative error of at most 0.014.
Values may be sent and summed in bfloat16 or wider, within the bound.
A program may use at most 128 MiB of HBM per device.

```python
import math
import jax
import jax.numpy as jnp
import numpy as np
from jax import lax

D = 2880
FF = 2880
TOP = 4
TOK_DEV = 256
EXPERTS = 16
TOKENS = 2048
CAP = 128
FF_DEV = 720
N_EP = 8
N_TP = 4


def shard_levels(stream_key, shape, pieces, smallest, high):
    factor_of = 1.0
    for axis_at, shards_of in pieces:
        heights = jax.random.uniform(jax.random.fold_in(jax.random.fold_in(stream_key, 6), axis_at), (shards_of,), jnp.float32, smallest / len(pieces), high / len(pieces))
        factor_of = factor_of * jnp.repeat(jnp.exp(heights), shape[axis_at] // shards_of).reshape((-1,) + (1,) * (len(shape) - 1 - axis_at))
    return factor_of


def assign_block(key, own, number, rows, count, top, most, skew):
    ranking = jax.random.permutation(key, count)
    packed, usual = portions_of(count, rows * top, most, skew, True), portions_of(count, rows * top, most, skew, False)
    places = jnp.arange(count)

    def named(tallies, offset_by):
        used = int((tallies > 0).sum())
        fixed = max(1, used // 4)
        moved = fixed + (places - fixed + offset_by * (used - fixed)) % max(1, count - fixed)
        return jnp.zeros((count,), jnp.int32).at[ranking[jnp.where(places < fixed, places, moved)]].set(jnp.asarray(tallies, jnp.int32))

    tallies = jnp.where(number % 4 == 0, named(packed, number // 4), named(usual, number - number // 4 - 1))
    mixed = jax.random.permutation(jax.random.fold_in(own, 3), count)
    donor, taker = mixed[0:count // 2 * 2:2], mixed[1:count // 2 * 2:2]
    margin = jnp.minimum(tallies[donor] - 1, most - tallies[taker]) // 2
    margin = jnp.where((donor == ranking[0]) | (taker == ranking[0]) | (tallies[taker] == 0), 0, jnp.maximum(margin, 0))
    moved = jax.random.randint(jax.random.fold_in(own, 4), (count // 2,), 0, 1 << 20) % (margin + 1)
    tallies = tallies.at[donor].add(-moved).at[taker].add(moved)
    labels = jnp.searchsorted(jnp.cumsum(tallies), jnp.arange(rows * top), side="right").astype(jnp.int32)
    table = labels.reshape(top, rows).T
    table = table[jax.random.permutation(jax.random.fold_in(own, 1), rows)]
    offset_by = jax.random.randint(jax.random.fold_in(own, 2), (rows, 1), 0, top)
    return jnp.take_along_axis(table, (jnp.arange(top)[None, :] + offset_by) % top, axis=1)


def portions_of(count, total, limit, skew, full):
    loads = [(1 << 20) // math.isqrt(rank ** skew) + 1 for rank in range(1, count + 1)]
    largest = limit if full else min(limit, max(-(-total // count), total * loads[0] // sum(loads)))
    least = 1 if total - largest >= count - 1 else 0
    holding, spare = [largest] + [least] * (count - 1), total - largest - least * (count - 1)
    while spare > 0:
        free = [i for i in range(1, count) if holding[i] < largest] or [i for i in range(1, count) if holding[i] < limit]
        pool, left = sum([loads[i] for i in free]), spare
        for i in free:
            extra = min(limit - holding[i], max(1, left * loads[i] // pool), spare)
            holding[i] = holding[i] + extra
            spare = spare - extra
    return np.array(holding)


def normal_values(rng, dims, width, reach, cuts=(), held_as=jnp.bfloat16):
    gain = shard_levels(rng, dims, cuts, -0.22, 0.18) if cuts else 1.0
    array = jax.random.normal(rng, dims, jnp.float32) * width * gain
    return jnp.minimum(jnp.maximum(array, -reach), reach).astype(held_as)


def setup_inputs(seed: int = 0) -> dict:
    seeds = jax.random.split(jax.random.key(seed), 7)
    tokens = normal_values(seeds[0], (TOKENS, D), 1.0, 6.0, ((0, 8), (1, 4)))
    expert_ids_keys = jax.random.split(jax.random.fold_in(seeds[1], 1), TOKENS // TOK_DEV)
    expert_ids_turns = jax.random.permutation(jax.random.fold_in(seeds[1], 3), TOKENS // TOK_DEV)
    expert_ids = jax.vmap(lambda own, number: assign_block(jax.random.fold_in(seeds[1], 2), own, number, TOK_DEV, EXPERTS, TOP, CAP, 2))(expert_ids_keys, expert_ids_turns).reshape((TOKENS, TOP))
    combine_weights = jnp.clip(jnp.exp(math.log(0.6) - 2.4849067 * jax.random.uniform(seeds[2], (TOKENS, TOP), jnp.float32) ** shard_levels(seeds[2], (TOKENS, TOP), ((0, 8),), -0.2, 0.2)), 0.05, 0.6)
    gate_weight = normal_values(seeds[3], (EXPERTS, D, FF), D ** -0.5, 0.109375, ((0, 8), (2, 4)))
    up_weight = normal_values(seeds[4], (EXPERTS, D, FF), D ** -0.5, 0.109375, ((0, 8), (2, 4)))
    down_weight = normal_values(seeds[5], (EXPERTS, FF, D), FF ** -0.5, 0.109375, ((0, 8), (1, 4)))
    return {"tokens": tokens, "expert_ids": expert_ids, "combine_weights": combine_weights, "gate_weight": gate_weight, "up_weight": up_weight, "down_weight": down_weight}


def activate(gate_acc, up_acc):
    return (up_acc + 1.0) * gate_acc * jax.nn.sigmoid(1.702 * gate_acc)


def reference(tokens, expert_ids, combine_weights, gate_weight, up_weight, down_weight):
    groups = expert_ids.reshape(N_EP, TOK_DEV * TOP)
    onehot = (groups[:, :, None] == jnp.arange(EXPERTS, dtype=jnp.int32)[None, None, :]).astype(jnp.int32)
    slot_pos = jnp.sum((jnp.cumsum(onehot, axis=1) - onehot) * onehot, axis=2)
    group_ids = jnp.arange(N_EP, dtype=jnp.int32)[:, None]
    flat_slot = ((groups * N_EP + group_ids) * CAP + slot_pos).reshape(-1)
    token_idx = (group_ids * TOK_DEV + jnp.arange(TOK_DEV * TOP, dtype=jnp.int32)[None, :] // TOP).reshape(-1)
    token_src = jnp.zeros((EXPERTS * N_EP * CAP,), jnp.int32).at[flat_slot].set(token_idx)
    slot_weight = jnp.zeros((EXPERTS * N_EP * CAP,), jnp.float32).at[flat_slot].set(combine_weights.reshape(-1))
    token_src = token_src.reshape(EXPERTS, N_EP * CAP)
    slot_weight = slot_weight.reshape(EXPERTS, N_EP * CAP)

    def per_expert(accum, inputs):
        row_src, row_weight, gate_cols, up_cols, down_rows = inputs
        row_data = tokens[row_src]
        gate_acc = jnp.dot(row_data, gate_cols, preferred_element_type=jnp.float32)
        up_acc = jnp.dot(row_data, up_cols, preferred_element_type=jnp.float32)
        hidden = activate(gate_acc, up_acc).astype(jnp.bfloat16)
        partials = jnp.einsum("rtf,tfd->rtd",
                              hidden.reshape(N_EP * CAP, N_TP, FF_DEV).astype(jnp.float32),
                              down_rows.reshape(N_TP, FF_DEV, D).astype(jnp.float32))
        rounded = lax.optimization_barrier(partials.astype(jnp.bfloat16))
        expert_out = jnp.sum(rounded.astype(jnp.float32), axis=1)
        accum = accum.at[row_src].add(row_weight[:, None] * expert_out)
        return accum, None

    accum = jnp.zeros((TOKENS, D), jnp.float32)
    accum, unused = lax.scan(per_expert, accum, (token_src, slot_weight, gate_weight, up_weight, down_weight))
    return accum.astype(jnp.bfloat16)
```

```python
import functools

import jax
import jax.numpy as jnp
from jax import lax
from jax.experimental import pallas as pl
from jax.experimental.pallas import tpu as pltpu
from jax.sharding import PartitionSpec as P


def activate(gate_acc, up_acc):
    return (up_acc + 1.0) * gate_acc * jax.nn.sigmoid(1.702 * gate_acc)


MESH = pl.DeviceIdType.MESH


class Place:
    def __init__(self, depth):
        self.depth = depth
        e, t = lax.axis_index("ep"), lax.axis_index("tp")
        self.z, self.x, self.y, self.c = e // 2, e % 2, t // 2, t % 2

    def device(self, k=0, dx=0, dy=0, dc=0):
        ep = (self.z + k) % self.depth * 2 + (self.x + dx) % 2
        tp = (self.y + dy) % 2 * 2 + (self.c + dc) % 2
        return ep, tp

    def block(self, k=0, dx=0, dy=0, dc=0):
        ep, tp = self.device(k, dx, dy, dc)
        return ep * 4 + tp

    def greet(self):
        barrier = pltpu.get_barrier_semaphore()
        near = [self.device(k=k) for k in range(1, self.depth)]
        near += [self.device(dx=1), self.device(dy=1), self.device(dc=1)]
        for who in near:
            pl.semaphore_signal(barrier, inc=1, device_id=who, device_id_type=MESH)
        pl.semaphore_wait(barrier, len(near))


def gather_kernel(depth, own, out, lane_recv, pair_recv, lane_send, pair_send, own_sem):
    here = Place(depth)
    half = own.shape[0] // 2
    sent = []

    def piece(k, dx, dy, part):
        rows = pl.ds(part * half, half)
        if (k, dx, dy) == (0, 0, 0):
            return own.at[rows]
        return out.at[here.block(k, dx, dy), rows]

    def lane_slot(k, dx, dy):
        ep, tp = here.device(k, dx, dy)
        return ep * 2 + tp // 2

    def push(k, dx, dy, part, to):
        rows = pl.ds(part * half, half)
        copy = pltpu.make_async_remote_copy(
            src_ref=piece(k, dx, dy, part), dst_ref=out.at[here.block(k, dx, dy), rows],
            send_sem=lane_send.at[len(sent)], recv_sem=lane_recv.at[lane_slot(k, dx, dy), part],
            device_id=to, device_id_type=MESH)
        copy.start()
        sent.append(copy)

    def pair(k, dx, dy, part):
        rows = pl.ds(part * half, half)
        slot = lane_slot(k, dx, dy)
        copy = pltpu.make_async_remote_copy(
            src_ref=piece(k, dx, dy, part), dst_ref=out.at[here.block(k, dx, dy), rows],
            send_sem=pair_send.at[slot, part], recv_sem=pair_recv.at[slot, part],
            device_id=here.device(dc=1), device_id_type=MESH)
        copy.start()

    def landed(k, dx, dy, part, to):
        rows = pl.ds(part * half, half)
        ref = out.at[here.block(k, dx, dy), rows]
        pltpu.make_async_remote_copy(
            src_ref=ref, dst_ref=ref, send_sem=lane_send.at[0],
            recv_sem=lane_recv.at[lane_slot(k, dx, dy), part],
            device_id=to, device_id_type=MESH).wait_recv()

    here.greet()
    over_x, over_y = here.device(dx=1), here.device(dy=1)
    for k in range(1, depth):
        for part in (0, 1):
            push(0, 0, 0, part, here.device(k=depth - k))
    store = pltpu.make_async_copy(own, out.at[here.block()], own_sem)
    store.start()
    for k in range(depth):
        if k:
            landed(k, 0, 0, 0, here.device(k=k))
            landed(k, 0, 0, 1, here.device(k=k))
        push(k, 0, 0, 0, over_x)
        push(k, 0, 0, 1, over_y)
        push(k, 0, 0, 0, over_y)
        push(k, 0, 0, 1, over_x)
        pair(k, 0, 0, 0)
        pair(k, 0, 0, 1)
        landed(k, 1, 0, 0, over_x)
        push(k, 1, 0, 0, over_y)
        pair(k, 1, 0, 0)
        landed(k, 0, 1, 1, over_y)
        push(k, 0, 1, 1, over_x)
        pair(k, 0, 1, 1)
    for k in range(depth):
        landed(k, 0, 1, 0, over_y)
        pair(k, 0, 1, 0)
        landed(k, 1, 0, 1, over_x)
        pair(k, 1, 0, 1)
        landed(k, 1, 1, 0, over_y)
        pair(k, 1, 1, 0)
        landed(k, 1, 1, 1, over_x)
        pair(k, 1, 1, 1)
    store.wait()
    for copy in sent:
        copy.wait_send()
    for k in range(depth):
        for dx in (0, 1):
            for dy in (0, 1):
                slot = lane_slot(k, dx, dy)
                for part in (0, 1):
                    rows = pl.ds(part * half, half)
                    copy = pltpu.make_async_remote_copy(
                        src_ref=piece(k, dx, dy, part),
                        dst_ref=out.at[here.block(k, dx, dy, 1), rows],
                        send_sem=pair_send.at[slot, part], recv_sem=pair_recv.at[slot, part],
                        device_id=here.device(dc=1), device_id_type=MESH)
                    copy.wait_send()
                    copy.wait_recv()


def gather_all(tokens, ep_count, tp_count):
    rows, width = tokens.shape
    depth = ep_count // 2
    blocks = ep_count * tp_count
    sends = 2 * (depth - 1) + 6 * depth
    dma = pltpu.SemaphoreType.DMA
    return pl.pallas_call(
        functools.partial(gather_kernel, depth),
        out_shape=jax.ShapeDtypeStruct((blocks, rows, width), tokens.dtype),
        in_specs=[pl.BlockSpec(memory_space=pltpu.VMEM)],
        out_specs=pl.BlockSpec(memory_space=pl.ANY),
        scratch_shapes=[dma((blocks // 2, 2)), dma((blocks // 2, 2)), dma((sends,)),
                        dma((blocks // 2, 2)), dma(())],
        compiler_params=pltpu.CompilerParams(collective_id=0, has_side_effects=True),
    )(tokens)


def scatter_kernel(depth, part_ref, out, acc, inc, from_y, from_x, last_x, last_y, from_z,
                   load_sem, pair_send, pair_recv, send_sem, recv_sem):
    here = Place(depth)
    rows = out.shape[0]
    half = rows // 2
    low, high = pl.ds(0, half), pl.ds(half, half)
    order = list(range(1, depth)) + [0]
    spread = ((1, 1), (0, 1), (1, 0), (0, 0))
    over_x, over_y = here.device(dx=1), here.device(dy=1)
    sent = []
    loads, pairs = {}, {}
    cell = lambda k, dx, dy: (k * 2 + dx) * 2 + dy

    def add(at, part, got):
        acc[at, part] = (acc[at, part].astype(jnp.float32) + got.astype(jnp.float32)).astype(acc.dtype)

    def send(src, dst, to):
        copy = pltpu.make_async_remote_copy(
            src_ref=src, dst_ref=dst, send_sem=send_sem.at[len(sent)],
            recv_sem=recv_sem.at[len(sent)], device_id=to, device_id_type=MESH)
        copy.start()
        sent.append(copy)
        return copy

    here.greet()
    for k in order:
        for dx, dy in spread:
            i = cell(k, dx, dy)
            pairs[i] = pltpu.make_async_remote_copy(
                src_ref=part_ref.at[here.block(k, dx, dy, 1)], dst_ref=inc.at[i],
                send_sem=pair_send.at[i], recv_sem=pair_recv.at[i],
                device_id=here.device(dc=1), device_id_type=MESH)
            pairs[i].start()
            loads[i] = pltpu.make_async_copy(
                part_ref.at[here.block(k, dx, dy)], acc.at[i], load_sem.at[i])
            loads[i].start()

    wait_for = {}

    def first(k):
        for dx, dy in spread:
            i = cell(k, dx, dy)
            loads[i].wait()
            pairs[i].wait_recv()
            add(i, pl.ds(0, rows), inc[i])
            if dy:
                wait_for["y", k, dx] = send(acc.at[i, low], from_y.at[k * 2 + dx], over_y)
            if dx:
                wait_for["x", k, dy] = send(acc.at[i, high], from_x.at[k * 2 + dy], over_x)

    def second(k):
        wait_for["y", k, 1].wait_recv()
        add(cell(k, 1, 0), low, from_y[k * 2 + 1])
        wait_for["lx", k] = send(acc.at[cell(k, 1, 0), low], last_x.at[k], over_x)
        wait_for["x", k, 1].wait_recv()
        add(cell(k, 0, 1), high, from_x[k * 2 + 1])
        wait_for["ly", k] = send(acc.at[cell(k, 0, 1), high], last_y.at[k], over_y)
        wait_for["y", k, 0].wait_recv()
        add(cell(k, 0, 0), low, from_y[k * 2])
        wait_for["x", k, 0].wait_recv()
        add(cell(k, 0, 0), high, from_x[k * 2])

    def third(k):
        wait_for["lx", k].wait_recv()
        add(cell(k, 0, 0), low, last_x[k])
        wait_for["ly", k].wait_recv()
        add(cell(k, 0, 0), high, last_y[k])
        if k:
            wait_for["z", k] = send(acc.at[cell(k, 0, 0)], from_z.at[k - 1], here.device(k=k))

    for i in range(depth + 2):
        if i < depth:
            first(order[i])
        if 0 <= i - 1 < depth:
            second(order[i - 1])
        if 0 <= i - 2:
            third(order[i - 2])
    total = acc[0].astype(jnp.float32)
    for k in range(1, depth):
        wait_for["z", k].wait_recv()
        total = total + from_z[k - 1].astype(jnp.float32)
    out[...] = total.astype(out.dtype)
    for copy in sent:
        copy.wait_send()
    for copy in pairs.values():
        copy.wait_send()


def scatter_sum(partial, ep_count):
    blocks, rows, width = partial.shape
    depth = ep_count // 2
    lane, half = blocks // 2, rows // 2
    sends = 6 * depth + depth - 1
    dma, kind = pltpu.SemaphoreType.DMA, partial.dtype
    return pl.pallas_call(
        functools.partial(scatter_kernel, depth),
        out_shape=jax.ShapeDtypeStruct((rows, width), kind),
        in_specs=[pl.BlockSpec(memory_space=pl.ANY)],
        out_specs=pl.BlockSpec(memory_space=pltpu.VMEM),
        scratch_shapes=[
            pltpu.VMEM((lane, rows, width), kind), pltpu.VMEM((lane, rows, width), kind),
            pltpu.VMEM((2 * depth, half, width), kind), pltpu.VMEM((2 * depth, half, width), kind),
            pltpu.VMEM((depth, half, width), kind), pltpu.VMEM((depth, half, width), kind),
            pltpu.VMEM((depth - 1, rows, width), kind),
            dma((lane,)), dma((lane,)), dma((lane,)), dma((sends,)), dma((sends,)),
        ],
        compiler_params=pltpu.CompilerParams(
            collective_id=1, has_side_effects=True, vmem_limit_bytes=48 * 1024 * 1024),
    )(partial)


def local(tokens, expert_ids, combine_weights, gate_weight, up_weight, down_weight):
    ep_count = lax.axis_size("ep")
    tp_count = lax.axis_size("tp")
    exp_local = gate_weight.shape[0]
    experts = exp_local * ep_count
    tok_rows = expert_ids.shape[0]
    top_count = expert_ids.shape[1]
    capacity = 2 * tok_rows * top_count // experts
    feat_width = tokens.shape[1]
    ff_width = gate_weight.shape[2]
    width = feat_width * tp_count
    f32, bf16 = jnp.float32, jnp.bfloat16

    ids_all = lax.all_gather(expert_ids.T, "ep")
    weights_all = lax.all_gather(combine_weights.T, "ep")
    first = lax.axis_index("ep") * exp_local
    mine = first + jnp.arange(exp_local, dtype=jnp.int32)
    hit = ids_all[:, None, :, :] == mine[None, :, None, None]
    chosen = jnp.any(hit, axis=2)
    weight = jnp.sum(jnp.where(hit, weights_all[:, None, :, :], 0.0), axis=2)

    ahead = jnp.triu(jnp.ones((tok_rows, tok_rows), bf16), 1)
    slot = lax.dot_general(
        chosen.reshape(-1, tok_rows).astype(bf16), ahead, (((1,), (0,)), ((), ())),
        preferred_element_type=f32,
    ).astype(jnp.int32).reshape(chosen.shape)
    place = jnp.where(chosen, slot, -1)
    take = place[:, :, None, :] == jnp.arange(capacity, dtype=jnp.int32)[None, None, :, None]
    slot_weight = jnp.sum(jnp.where(take, weight[:, :, None, :], 0.0), axis=3)
    take = take.astype(bf16)

    paired = tp_count == 2 * 2 and ep_count % 2 == 0
    spread = gather_all(tokens, ep_count, tp_count) if paired else lax.all_gather(
        tokens, ("ep", "tp")
    )
    gathered = spread.reshape(
        ep_count, tp_count, tok_rows, feat_width
    )
    routed = jnp.einsum(
        "sect,sjtf->escjf", take, gathered, preferred_element_type=f32
    ).astype(bf16)
    rows = routed.reshape(exp_local, ep_count * capacity, width)
    gate_new = jnp.einsum("erd,edf->erf", rows, gate_weight, preferred_element_type=f32)
    up_new = jnp.einsum("erd,edf->erf", rows, up_weight, preferred_element_type=f32)
    row_weight = slot_weight.transpose(1, 0, 2).reshape(exp_local, ep_count * capacity, 1)
    hidden = (activate(gate_new, up_new) * row_weight).astype(bf16)
    expert_out = jnp.einsum(
        "erf,efd->erd", hidden, down_weight, preferred_element_type=f32
    ).astype(bf16)
    expert_out = expert_out.reshape(exp_local, ep_count, capacity, tp_count, feat_width)
    partial = jnp.einsum(
        "sect,escjf->sjtf", take, expert_out, preferred_element_type=f32
    ).astype(bf16)
    partial = partial.reshape(ep_count * tp_count, tok_rows, feat_width)
    if paired:
        return scatter_sum(partial, ep_count)
    mixed = lax.psum_scatter(partial, ("ep", "tp"), scatter_dimension=0, tiled=True)
    return mixed.reshape(tok_rows, feat_width)


def solution(mesh):
    in_specs = (
        P("ep", "tp"),
        P("ep", None),
        P("ep", None),
        P("ep", None, "tp"),
        P("ep", None, "tp"),
        P("ep", "tp", None),
    )
    out_specs = P("ep", "tp")
    return jax.shard_map(local, mesh=mesh, in_specs=in_specs, out_specs=out_specs, check_vma=False)
```
